32 devices in a mesh: patch: 16 (over z, y, x), width: 2 (over core).
Axes of the slice: x: 2, y: 2, z: 4, core: 2. Of those that a mesh axis runs over, the one named last changes fastest.
Arguments:
- node_latents: bfloat16 [512, 2048], P('width', 'patch'), may hold values from -6 to 6
- edge_latents: bfloat16 [512, 16384], P('width', 'patch'), may hold values from -6 to 6
- senders: int32 [16384], P('patch'), may hold values from 0 to 2047, as said below
- receivers: int32 [16384], P('patch'), may hold values from 0 to 2047, as said below
- edge_count: int32 [16], P('patch'), may hold values from 512 to 1024, as said below
- edge_in_weight: bfloat16 [2, 512, 1536], P(None, 'width'), may hold values from -0.15625 to 0.15625
- edge_in_bias: float32 [2, 512], P(None, 'width'), may hold values from -3 to 3
- edge_out_weight: bfloat16 [2, 512, 512], P(None, 'width'), may hold values from -0.25 to 0.25
- edge_out_bias: float32 [2, 512], P(None, 'width'), may hold values from -3 to 3
- edge_gain: float32 [2, 512], P(None, 'width'), may hold values from 0.1 to 1.9
- edge_shift: float32 [2, 512], P(None, 'width'), may hold values from -3 to 3
- node_in_weight: bfloat16 [2, 512, 1024], P(None, 'width'), may hold values from -0.1875 to 0.1875
- node_in_bias: float32 [2, 512], P(None, 'width'), may hold values from -3 to 3
- node_out_weight: bfloat16 [2, 512, 512], P(None, 'width'), may hold values from -0.25 to 0.25
- node_out_bias: float32 [2, 512], P(None, 'width'), may hold values from -3 to 3
- node_gain: float32 [2, 512], P(None, 'width'), may hold values from 0.1 to 1.9
- node_shift: float32 [2, 512], P(None, 'width'), may hold values from -3 to 3
Outputs:
- nodes_out: bfloat16 [512, 2048], P('width', 'patch')
- edges_out: bfloat16 [512, 16384], P('width', 'patch')
The draws below stay inside these ranges and needn't reach their ends.
Inputs may be any that keep to these rules, and one draw needn't show every extreme that they name: `senders`: the sender of a slot of patch p is a node of patch p, of patch p - 1 or p + 1 (counted around, modulo the number of patches), or one of the first 16 nodes of some patch. `receivers`: row r names a node of patch r // 1024, from (r // 1024) * 128 to that plus 128 - 1. Slots p * 1024 to p * 1024 + edge_count[p] - 1 of patch p are live, the rest are padding; some patch has all 1024 slots live.
All inputs are finite; a program needn't handle non-finite values.
Results may differ from the reference program's by a relative error of at most 0.014.
Values may be sent and summed in bfloat16 or wider, within the bound.
A program may use at most 64 MiB of HBM per device.

```python
import jax
import jax.numpy as jnp
from jax import lax

D = 512
H = 512
LAYERS = 2
NODE_DEV = 128
COARSE = 16
EDGE_DEV = 1024
NODES = 2048
EDGES = 16384


def draw_graph(key):
    base = jax.random.fold_in(key, 17)
    keys = jax.random.split(base, 8)
    patches = NODES // NODE_DEV
    slots = jnp.arange(EDGES, dtype=jnp.int32)
    block = slots // EDGE_DEV
    local = jax.random.randint(keys[0], (EDGES,), 0, NODE_DEV).astype(jnp.int32)
    receivers = block * NODE_DEV + local
    kinds = jax.random.randint(keys[1], (EDGES,), 0, 4)
    offset = jax.random.randint(keys[2], (EDGES,), -8, 9).astype(jnp.int32)
    near = block * NODE_DEV + (local + offset) % NODE_DEV
    sideways = jax.random.randint(keys[3], (EDGES,), 0, 2).astype(jnp.int32) * 2 - 1
    beside = (block + sideways) % patches * NODE_DEV + jax.random.randint(keys[4], (EDGES,), 0, NODE_DEV).astype(jnp.int32)
    random_patch = jax.random.randint(keys[5], (EDGES,), 0, patches).astype(jnp.int32)
    opposite = ((block + patches // 2) % patches).astype(jnp.int32)
    toward = jax.random.randint(keys[7], (EDGES,), 0, 2)
    far_patch = jnp.where(toward == 1, opposite, random_patch)
    anywhere = far_patch * NODE_DEV + jax.random.randint(keys[6], (EDGES,), 0, COARSE).astype(jnp.int32)
    senders = jnp.where(kinds < 2, near, jnp.where(kinds == 2, beside, anywhere))
    return (senders.astype(jnp.int32), receivers.astype(jnp.int32))


def draw_senders(key, part):
    return draw_graph(key)[0]


def draw_receivers(key, part):
    return draw_graph(key)[1]


def draw_edge_count(key, part):
    patches = NODES // NODE_DEV
    first, second = jax.random.split(jax.random.fold_in(key, 29))
    counts = jax.random.randint(first, (patches,), EDGE_DEV // 2, EDGE_DEV + 1).astype(jnp.int32)
    filled = jax.random.randint(second, (), 0, patches)
    return jnp.where(jnp.arange(patches) == filled, EDGE_DEV, counts).astype(jnp.int32)


def levels(rng, extent, shards, low, largest):
    def one(dim, shards_of):
        draws = jax.random.uniform(jax.random.fold_in(jax.random.fold_in(rng, 6), dim), (shards_of,), jnp.float32, low / len(shards), largest / len(shards))
        return jnp.repeat(jnp.exp(draws), extent[dim] // shards_of).reshape((-1,) + (1,) * (len(extent) - dim - 1))

    level = one(*shards[0])
    for cut in shards[1:]:
        level = level * one(*cut)
    return level


def gaussian(rng, shape, width, bound, shards=(), held_as=jnp.bfloat16):
    drawn = width * jax.random.normal(rng, shape, jnp.float32)
    if shards:
        drawn = drawn * levels(rng, shape, shards, -0.22, 0.18)
    return jnp.clip(drawn, -bound, bound).astype(held_as)


def setup_inputs(seed: int = 0) -> dict:
    key_of = jax.random.split(jax.random.key(seed), 18)
    return {
        "node_latents": gaussian(key_of[0], (D, NODES), 1.0, 6.0, ((0, 2), (1, 16))),
        "edge_latents": gaussian(key_of[1], (D, EDGES), 1.0, 6.0, ((0, 2), (1, 16))),
        "senders": draw_senders(jax.random.fold_in(key_of[17], 71), 0),
        "receivers": draw_receivers(jax.random.fold_in(key_of[17], 71), 0),
        "edge_count": draw_edge_count(jax.random.fold_in(key_of[17], 71), 0),
        "edge_in_weight": gaussian(key_of[5], (LAYERS, H, 3 * D), (3 * D) ** -0.5, 0.15625, ((1, 2),)),
        "edge_in_bias": gaussian(key_of[6], (LAYERS, H), 0.5, 3.0, ((1, 2),), jnp.float32),
        "edge_out_weight": gaussian(key_of[7], (LAYERS, H, D), H ** -0.5, 0.25, ((1, 2),)),
        "edge_out_bias": gaussian(key_of[8], (LAYERS, D), 0.5, 3.0, ((1, 2),), jnp.float32),
        "edge_gain": jnp.clip(1.0 + 0.18 * jax.random.normal(key_of[9], (LAYERS, D), jnp.float32), 0.1, 1.9),
        "edge_shift": gaussian(key_of[10], (LAYERS, D), 0.5, 3.0, ((1, 2),), jnp.float32),
        "node_in_weight": gaussian(key_of[11], (LAYERS, H, 2 * D), (2 * D) ** -0.5, 0.1875, ((1, 2),)),
        "node_in_bias": gaussian(key_of[12], (LAYERS, H), 0.5, 3.0, ((1, 2),), jnp.float32),
        "node_out_weight": gaussian(key_of[13], (LAYERS, H, D), H ** -0.5, 0.25, ((1, 2),)),
        "node_out_bias": gaussian(key_of[14], (LAYERS, D), 0.5, 3.0, ((1, 2),), jnp.float32),
        "node_gain": jnp.clip(1.0 + 0.18 * jax.random.normal(key_of[15], (LAYERS, D), jnp.float32), 0.1, 1.9),
        "node_shift": gaussian(key_of[16], (LAYERS, D), 0.5, 3.0, ((1, 2),), jnp.float32),
    }


def layer_norm(values, gain, shift):
    mean = lax.optimization_barrier(jnp.sum(values, axis=-1, keepdims=True)) / D
    square = lax.optimization_barrier(jnp.sum(values * values, axis=-1, keepdims=True)) / D
    return (values - mean) * jax.lax.rsqrt(square - mean * mean + 1e-05) * gain + shift

def reference(node_latents, edge_latents, senders, receivers, edge_count, edge_in_weight, edge_in_bias, edge_out_weight, edge_out_bias, edge_gain, edge_shift, node_in_weight, node_in_bias, node_out_weight, node_out_bias, node_gain, node_shift):
    slots = jnp.arange(EDGES, dtype=jnp.int32)
    live = slots % EDGE_DEV < edge_count[slots // EDGE_DEV]
    nodes = node_latents.T
    edges = edge_latents.T
    for layer in range(LAYERS):
        w_edge = edge_in_weight[layer].T
        w_node = node_in_weight[layer].T
        sender_part = jnp.dot(nodes, w_edge[D:2 * D], preferred_element_type=jnp.float32).astype(jnp.bfloat16)
        receiver_part = jnp.dot(nodes, w_edge[2 * D:], preferred_element_type=jnp.float32).astype(jnp.bfloat16)
        node_first = jnp.dot(nodes, w_node[:D], preferred_element_type=jnp.float32)
        before = jnp.dot(edges, w_edge[:D], preferred_element_type=jnp.float32)
        before = before + sender_part[senders].astype(jnp.float32) + receiver_part[receivers].astype(jnp.float32) + edge_in_bias[layer]
        edge_hidden = jax.nn.silu(before).astype(jnp.bfloat16)
        edge_mlp = jnp.dot(edge_hidden, edge_out_weight[layer], preferred_element_type=jnp.float32) + edge_out_bias[layer]
        updated = edges.astype(jnp.float32) + layer_norm(edge_mlp, edge_gain[layer], edge_shift[layer])
        edges = jnp.where(live[:, None], updated, jnp.float32(0.0)).astype(jnp.bfloat16)
        aggregate = jax.ops.segment_sum(edges.astype(jnp.float32), receivers, num_segments=NODES).astype(jnp.bfloat16)
        node_before = node_first + jnp.dot(aggregate, w_node[D:], preferred_element_type=jnp.float32) + node_in_bias[layer]
        node_hidden = jax.nn.silu(node_before).astype(jnp.bfloat16)
        node_mlp = jnp.dot(node_hidden, node_out_weight[layer], preferred_element_type=jnp.float32) + node_out_bias[layer]
        nodes = (nodes.astype(jnp.float32) + layer_norm(node_mlp, node_gain[layer], node_shift[layer])).astype(jnp.bfloat16)
    return (nodes.T, edges.T)
```

```python
import functools

import jax
import jax.numpy as jnp
from jax import lax
from jax.experimental import pallas as pl
from jax.experimental.pallas import tpu as pltpu
from jax.sharding import PartitionSpec as P

MESH = pl.DeviceIdType.MESH
epsilon = 1e-05
bf16 = jnp.bfloat16
f32 = jnp.float32


def dot(left, right, dims=((1,), (0,))):
    return lax.dot_general(left, right, (dims, ((), ())), preferred_element_type=f32)


def silu(v):
    h = 0.5 * v
    return h + h * jnp.tanh(h)


def layer_norm(values, gain, shift):
    width = values.shape[0]
    mean = jnp.sum(values, axis=0, keepdims=True) / width
    square = jnp.sum(values * values, axis=0, keepdims=True) / width
    return (values - mean) * lax.rsqrt(square - mean * mean + epsilon) * gain + shift


def kernel(
    patches,
    nodes_in,
    edges_in,
    senders_ref,
    receivers_ref,
    count_ref,
    wi_in,
    wo_in,
    vi_in,
    vo_in,
    *rest,
):
    vector_in = rest[:8]
    nodes_out, edges_out = rest[8:10]
    (
        nodes,
        edges,
        wi,
        wo,
        vi,
        vo,
        vectors,
        columns,
        halo,
        coarse,
        part_send,
        coarse_send,
        agg_send,
        agg_recv,
        own,
        hot_own,
        hot_halo,
        hot_coarse,
        incidence,
        before,
        local_sem,
        w_send,
        w_recv,
        halo_send,
        halo_recv,
        coarse_send_sem,
        coarse_recv_sem,
        relay_send,
        relay_recv,
        agg_sems,
        out_sems,
    ) = rest[10:]
    layers = wi.shape[0]
    half = nodes_in.shape[0]
    width = 2 * half
    rows = nodes_in.shape[1]
    slots = edges_in.shape[1]
    mine = slots // 2
    top = coarse_send.shape[1]
    far = patches - 3

    me = lax.axis_index("patch")
    core = lax.axis_index("width")
    other = 1 - core
    here = pl.ds(pl.multiple_of(core * half, half), half)
    there = pl.ds(pl.multiple_of(other * half, half), half)
    my_slots = pl.ds(pl.multiple_of(core * mine, mine), mine)
    other_slots = pl.ds(pl.multiple_of(other * mine, mine), mine)

    def local(src, dst, index):
        return pltpu.make_async_copy(src, dst, local_sem.at[index])

    def remote(src, dst, send, recv, patch, width_index):
        return pltpu.make_async_remote_copy(
            src_ref=src,
            dst_ref=dst,
            send_sem=send,
            recv_sem=recv,
            device_id={"patch": patch, "width": width_index},
            device_id_type=MESH,
        )

    blocks = [
        (nodes_in, nodes.at[here], nodes_in, nodes.at[there]),
        (edges_in.at[:, my_slots], edges.at[here], edges_in.at[:, other_slots], edges.at[there]),
    ]
    place = {"nodes": 0, "edges": 1}
    for layer in range(layers):
        for name, source, target in (("wi", wi_in, wi), ("wo", wo_in, wo), ("vi", vi_in, vi), ("vo", vo_in, vo)):
            place[name, layer] = len(blocks)
            blocks.append(
                (source.at[layer], target.at[layer, here], source.at[layer], target.at[layer, there])
            )
        if layer == 0:
            place["vectors"] = len(blocks)
            for index, source in enumerate(vector_in):
                blocks.append(
                    (source, vectors.at[index, :, here], source, vectors.at[index, :, there])
                )

    locals_ = [local(b[0], b[1], i) for i, b in enumerate(blocks)]
    for copy in locals_:
        copy.start()

    def greet(step, carry):
        target = lax.rem(me + step, patches)
        pl.semaphore_signal(
            pltpu.get_barrier_semaphore(), inc=1, device_id={"patch": target, "width": core}, device_id_type=MESH
        )
        return carry

    barrier = pltpu.get_barrier_semaphore()
    pl.semaphore_signal(barrier, inc=1, device_id={"patch": me, "width": other}, device_id_type=MESH)
    lax.fori_loop(1, patches, greet, 0)

    sender = senders_ref[:, my_slots]
    receiver = receivers_ref[:, my_slots] - me * rows
    slot = lax.broadcasted_iota(jnp.int32, (1, mine), 1) + core * mine
    live = slot < count_ref[0]
    owner = sender // rows
    within = sender - owner * rows
    distance = lax.rem(me - owner + patches, patches)
    node_iota = lax.broadcasted_iota(jnp.int32, (rows, mine), 0)

    def hot(index, iota):
        return jnp.where(iota == index, 1.0, 0.0).astype(bf16)

    hot_own[:rows] = hot(jnp.where(distance == 0, within, -1), node_iota)
    hot_own[rows:] = hot(receiver, node_iota)
    hot_halo[:rows] = hot(jnp.where(distance == 1, within, -1), node_iota)
    hot_halo[rows:] = hot(jnp.where(distance == patches - 1, within, -1), node_iota)
    far_index = jnp.where((distance >= 2) & (distance <= patches - 2), (distance - 2) * top + within, -1)
    hot_coarse[...] = hot(far_index, lax.broadcasted_iota(jnp.int32, hot_coarse.shape, 0))
    incidence[...] = hot(jnp.where(live, receiver, -1), node_iota)
    pad = coarse.shape[2] - far * top
    if pad:
        for layer in range(layers):
            for part in range(2):
                coarse[layer, part, far * top :, :] = jnp.zeros((pad, half), bf16)

    pl.semaphore_wait(barrier, patches)

    remotes = []
    for i, b in enumerate(blocks):
        target = b[1]
        remotes.append(remote(b[2], target, w_send.at[i], w_recv.at[i], me, other))
    for copy in remotes:
        copy.start()

    def arrive(index):
        locals_[index].wait()
        b = blocks[index]
        remote(b[3], b[3], w_send.at[index], w_recv.at[index], me, other).wait_recv()

    def column(index, layer):
        position = index * layers + layer
        return columns[:, position : position + 1]

    waited_out = []
    for layer in range(layers):
        if layer == 0:
            arrive(place["nodes"])
        locals_[place["wi", layer]].wait()
        part = dot(wi[layer, here, width : 2 * width], nodes[...])
        part_send[layer] = part.astype(bf16)
        up = remote(
            part_send.at[layer],
            halo.at[layer, here, pl.ds(0, rows)],
            halo_send.at[layer, 0],
            halo_recv.at[layer, 0],
            lax.rem(me + 1, patches),
            core,
        )
        down = remote(
            part_send.at[layer],
            halo.at[layer, here, pl.ds(rows, rows)],
            halo_send.at[layer, 1],
            halo_recv.at[layer, 1],
            lax.rem(me + patches - 1, patches),
            core,
        )
        up.start()
        down.start()
        coarse_send[layer] = part.T[:top].astype(bf16)

        def spread(step, carry):
            remote(
                coarse_send.at[layer],
                coarse.at[layer, core, pl.ds(pl.multiple_of((step - 2) * top, top), top)],
                coarse_send_sem.at[layer],
                coarse_recv_sem.at[layer],
                lax.rem(me + step, patches),
                core,
            ).start()
            return carry

        lax.fori_loop(2, patches - 1, spread, 0)

        b = blocks[place["wi", layer]]
        index = place["wi", layer]
        remote(b[3], b[3], w_send.at[index], w_recv.at[index], me, other).wait_recv()
        own[:, :rows] = dot(wi[layer, :, width : 2 * width], nodes[...]).astype(bf16)
        own[:, rows:] = dot(wi[layer, :, 2 * width :], nodes[...]).astype(bf16)
        if layer == 0:
            arrive(place["edges"])
            for k in range(8):
                arrive(place["vectors"] + k)
            flat = vectors[...].reshape(8 * layers, width)
            columns[...] = flat.T
        before[...] = (
            dot(wi[layer, :, :width], edges[...]) + dot(own[...], hot_own[...]) + column(0, layer)
        )
        arrive(place["vi", layer])
        node_first = dot(vi[layer, :, :width], nodes[...]) + column(4, layer)

        up.wait_recv()
        down.wait_recv()
        relay_halo = remote(
            halo.at[layer, here], halo.at[layer, here], relay_send.at[layer, 0], relay_recv.at[layer, 0], me, other
        )
        relay_halo.start()
        every = coarse.at[layer, core, pl.ds(0, far * top)]
        all_coarse = remote(every, every, coarse_send_sem.at[layer], coarse_recv_sem.at[layer], me, other)
        all_coarse.wait_recv()
        relay_coarse = remote(
            every, every, relay_send.at[layer, 1], relay_recv.at[layer, 1], me, other
        )
        relay_coarse.start()
        before[here, :] = (
            before[here, :]
            + dot(halo[layer, here, :], hot_halo[...])
            + dot(coarse[layer, core], hot_coarse[...], ((0,), (0,)))
        )
        arrive(place["wo", layer])
        from_halo = halo.at[layer, there]
        remote(from_halo, from_halo, relay_send.at[layer, 0], relay_recv.at[layer, 0], me, other).wait_recv()
        from_coarse = coarse.at[layer, other, pl.ds(0, far * top)]
        remote(from_coarse, from_coarse, relay_send.at[layer, 1], relay_recv.at[layer, 1], me, other).wait_recv()
        before[there, :] = (
            before[there, :]
            + dot(halo[layer, there, :], hot_halo[...])
            + dot(coarse[layer, other], hot_coarse[...], ((0,), (0,)))
        )

        hidden = silu(before[...]).astype(bf16)
        mlp = dot(wo[layer], hidden, ((0,), (0,))) + column(1, layer)
        updated = edges[...].astype(f32) + layer_norm(mlp, column(2, layer), column(3, layer))
        edges[...] = jnp.where(live, updated, 0.0).astype(bf16)
        partial = dot(edges[...], incidence[...], ((1,), (1,)))
        agg_send[layer] = partial.astype(bf16)
        swap = remote(
            agg_send.at[layer], agg_recv.at[layer], agg_sems.at[layer, 0], agg_sems.at[layer, 1], me, other
        )
        swap.start()
        if layer == layers - 1:
            keep = pltpu.make_async_copy(edges.at[here], edges_out.at[:, my_slots], out_sems.at[0])
            keep.start()
            give = remote(
                edges.at[there], edges_out.at[:, my_slots], out_sems.at[1], out_sems.at[2], me, other
            )
            give.start()
        arrive(place["vo", layer])
        swap.wait_recv()
        aggregate = (partial + agg_recv[layer].astype(f32)).astype(bf16)
        node_hidden = silu(node_first + dot(vi[layer, :, width:], aggregate)).astype(bf16)
        node_mlp = dot(vo[layer], node_hidden, ((0,), (0,))) + column(5, layer)
        nodes[...] = (
            nodes[...].astype(f32) + layer_norm(node_mlp, column(6, layer), column(7, layer))
        ).astype(bf16)
        waited_out += [up, down, all_coarse, relay_halo, relay_coarse, swap]

    store = pltpu.make_async_copy(nodes.at[here], nodes_out, out_sems.at[3])
    store.start()
    for copy in remotes + waited_out:
        copy.wait_send()
    keep.wait()
    give.wait_send()
    got = edges_out.at[:, other_slots]
    remote(got, got, out_sems.at[1], out_sems.at[2], me, other).wait_recv()
    store.wait()


def on_device(
    patches,
    node_latents,
    edge_latents,
    senders,
    receivers,
    edge_count,
    edge_in_weight,
    edge_in_bias,
    edge_out_weight,
    edge_out_bias,
    edge_gain,
    edge_shift,
    node_in_weight,
    node_in_bias,
    node_out_weight,
    node_out_bias,
    node_gain,
    node_shift,
):
    half, rows = node_latents.shape
    slots = edge_latents.shape[1]
    layers = edge_in_weight.shape[0]
    width = 2 * half
    mine = slots // 2
    top = rows // 8
    far_rows = -(-(patches - 3) * top // 128) * 128
    vmem = pltpu.VMEM
    dma = pltpu.SemaphoreType.DMA
    copies = 2 + 4 * layers + 8
    anywhere = pl.BlockSpec(memory_space=pl.ANY)
    return pl.pallas_call(
        functools.partial(kernel, patches),
        out_shape=(
            jax.ShapeDtypeStruct((half, rows), bf16),
            jax.ShapeDtypeStruct((half, slots), bf16),
        ),
        in_specs=[anywhere, anywhere]
        + [pl.BlockSpec(memory_space=vmem)] * 2
        + [pl.BlockSpec(memory_space=pltpu.SMEM)]
        + [anywhere] * 12,
        out_specs=(anywhere, anywhere),
        scratch_shapes=[
            vmem((width, rows), bf16),
            vmem((width, mine), bf16),
            vmem((layers, width, 3 * width), bf16),
            vmem((layers, width, width), bf16),
            vmem((layers, width, 2 * width), bf16),
            vmem((layers, width, width), bf16),
            vmem((8, layers, width), f32),
            vmem((width, 8 * layers), f32),
            vmem((layers, width, 2 * rows), bf16),
            vmem((layers, 2, far_rows, half), bf16),
            vmem((layers, half, rows), bf16),
            vmem((layers, top, half), bf16),
            vmem((layers, width, rows), bf16),
            vmem((layers, width, rows), bf16),
            vmem((width, 2 * rows), bf16),
            vmem((2 * rows, mine), bf16),
            vmem((2 * rows, mine), bf16),
            vmem((far_rows, mine), bf16),
            vmem((rows, mine), bf16),
            vmem((width, mine), f32),
            dma((copies,)),
            dma((copies,)),
            dma((copies,)),
            dma((layers, 2)),
            dma((layers, 2)),
            dma((layers,)),
            dma((layers,)),
            dma((layers, 2)),
            dma((layers, 2)),
            dma((layers, 2)),
            dma((4,)),
        ],
        compiler_params=pltpu.CompilerParams(collective_id=0, has_side_effects=True, vmem_limit_bytes=56 * 2**20),
    )(
        node_latents,
        edge_latents,
        senders.reshape(1, slots),
        receivers.reshape(1, slots),
        edge_count,
        edge_in_weight,
        edge_out_weight,
        node_in_weight,
        node_out_weight,
        edge_in_bias,
        edge_out_bias,
        edge_gain,
        edge_shift,
        node_in_bias,
        node_out_bias,
        node_gain,
        node_shift,
    )


def solution(mesh):
    by_width = P(None, "width")
    return jax.shard_map(
        functools.partial(on_device, mesh.shape["patch"]),
        mesh=mesh,
        in_specs=(
            P("width", "patch"),
            P("width", "patch"),
            P("patch"),
            P("patch"),
            P("patch"),
            P(None, "width", None),
            by_width,
            P(None, "width", None),
            by_width,
            by_width,
            by_width,
            P(None, "width", None),
            by_width,
            P(None, "width", None),
            by_width,
            by_width,
            by_width,
        ),
        out_specs=(P("width", "patch"), P("width", "patch")),
        check_vma=False,
    )
```

```python
import functools

import jax
import jax.numpy as jnp
from jax import lax
from jax.experimental import pallas as pl
from jax.experimental.pallas import tpu as pltpu
from jax.sharding import PartitionSpec as P

MESH = pl.DeviceIdType.MESH
epsilon = 1e-05
bf16 = jnp.bfloat16
f32 = jnp.float32


def dot(left, right, dims=((1,), (0,))):
    return lax.dot_general(left, right, (dims, ((), ())), preferred_element_type=f32)


def silu(v):
    h = 0.5 * v
    return h + h * jnp.tanh(h)


def layer_norm(values, gain, shift):
    width = values.shape[0]
    mean = jnp.sum(values, axis=0, keepdims=True) / width
    square = jnp.sum(values * values, axis=0, keepdims=True) / width
    return (values - mean) * lax.rsqrt(square - mean * mean + epsilon) * gain + shift


def kernel(
    patches,
    nodes_in,
    edges_in,
    senders_in,
    receivers_in,
    count_in,
    wi_in,
    wo_in,
    vi_in,
    vo_in,
    *rest,
):
    vector_in = rest[:8]
    nodes_out, edges_out = rest[8:10]
    (
        nodes,
        edges,
        wi,
        wo,
        vi,
        vo,
        vectors,
        columns,
        halo,
        coarse,
        part_send,
        coarse_send,
        agg_send,
        agg_recv,
        own,
        table,
        hot_own,
        hot_far,
        incidence,
        before,
        senders_ref,
        receivers_ref,
        count_ref,
        wo_turned,
        vo_turned,
        graph_sem,
        local_sem,
        w_send,
        w_recv,
        halo_send,
        halo_recv,
        coarse_send_sem,
        coarse_recv_sem,
        relay_send,
        relay_recv,
        agg_sems,
        out_sems,
    ) = rest[10:]
    layers = wi.shape[0]
    half = nodes_in.shape[0]
    width = 2 * half
    rows = nodes_in.shape[1]
    slots = edges_in.shape[1]
    mine = slots // 2
    top = coarse_send.shape[1]
    far = patches - 3

    me = lax.axis_index("patch")
    core = lax.axis_index("width")
    other = 1 - core
    here = pl.ds(pl.multiple_of(core * half, half), half)
    there = pl.ds(pl.multiple_of(other * half, half), half)
    my_slots = pl.ds(pl.multiple_of(core * mine, mine), mine)
    other_slots = pl.ds(pl.multiple_of(other * mine, mine), mine)

    def local(src, dst, index):
        return pltpu.make_async_copy(src, dst, local_sem.at[index])

    def remote(src, dst, send, recv, patch, width_index):
        return pltpu.make_async_remote_copy(
            src_ref=src,
            dst_ref=dst,
            send_sem=send,
            recv_sem=recv,
            device_id={"patch": patch, "width": width_index},
            device_id_type=MESH,
        )

    blocks = [
        (nodes_in, nodes.at[here], nodes_in, nodes.at[there]),
        (edges_in.at[:, my_slots], edges.at[here], edges_in.at[:, other_slots], edges.at[there]),
    ]
    place = {"nodes": 0, "edges": 1}
    for layer in range(layers):
        for name, source, target in (("wi", wi_in, wi), ("wo", wo_in, wo), ("vi", vi_in, vi), ("vo", vo_in, vo)):
            place[name, layer] = len(blocks)
            blocks.append(
                (source.at[layer], target.at[layer, here], source.at[layer], target.at[layer, there])
            )
        if layer == 0:
            place["vectors"] = len(blocks)
            for index, source in enumerate(vector_in):
                blocks.append(
                    (source, vectors.at[index, :, here], source, vectors.at[index, :, there])
                )

    def greet(step, carry):
        target = lax.rem(me + step, patches)
        pl.semaphore_signal(
            pltpu.get_barrier_semaphore(), inc=1, device_id={"patch": target, "width": core}, device_id_type=MESH
        )
        return carry

    barrier = pltpu.get_barrier_semaphore()
    pl.semaphore_signal(barrier, inc=1, device_id={"patch": me, "width": other}, device_id_type=MESH)
    lax.fori_loop(1, patches, greet, 0)

    graph = [
        pltpu.make_async_copy(source, target, graph_sem.at[i])
        for i, (source, target) in enumerate(
            ((senders_in, senders_ref), (receivers_in, receivers_ref), (count_in, count_ref))
        )
    ]
    locals_ = [local(b[0], b[1], i) for i, b in enumerate(blocks)]
    locals_[0].start()
    for copy in graph + locals_[1:]:
        copy.start()
    locals_[0].wait()
    coarse_send[0] = nodes[here, :].astype(f32).T[:top].astype(bf16)
    for copy in graph:
        copy.wait()

    sender = senders_ref[:, my_slots]
    receiver = receivers_ref[:, my_slots] - me * rows
    slot = lax.broadcasted_iota(jnp.int32, (1, mine), 1) + core * mine
    live = slot < count_ref[0]
    owner = sender // rows
    within = sender - owner * rows
    distance = lax.rem(me - owner + patches, patches)
    node_iota = lax.broadcasted_iota(jnp.int32, (rows, mine), 0)

    def hot(index, iota):
        return jnp.where(iota == index, 1.0, 0.0).astype(bf16)

    hot_own[:rows] = hot(jnp.where(distance == 0, within, -1), node_iota)
    hot_own[rows:] = hot(receiver, node_iota)
    hot_far[:rows] = hot(jnp.where(distance == 1, within, -1), node_iota)
    hot_far[rows : 2 * rows] = hot(jnp.where(distance == patches - 1, within, -1), node_iota)
    far_index = jnp.where((distance >= 2) & (distance <= patches - 2), (distance - 2) * top + within, -1)
    hot_far[2 * rows :] = hot(far_index, lax.broadcasted_iota(jnp.int32, (coarse.shape[2], mine), 0))
    incidence[...] = hot(jnp.where(live, receiver, -1), node_iota)
    pad = coarse.shape[2] - far * top
    if pad:
        for layer in range(layers):
            for part in range(2):
                coarse[layer, part, far * top :, :] = jnp.zeros((pad, half), bf16)

    pl.semaphore_wait(barrier, patches)

    def send_far(layer, source):
        copies = [
            remote(
                source,
                halo.at[layer, here, pl.ds(side * rows, rows)],
                halo_send.at[layer, side],
                halo_recv.at[layer, side],
                lax.rem(me + step, patches),
                core,
            )
            for side, step in enumerate((1, patches - 1))
        ]
        for copy in copies:
            copy.start()
        return copies

    def spread_coarse(layer):
        def spread(step, carry):
            remote(
                coarse_send.at[layer],
                coarse.at[layer, core, pl.ds(pl.multiple_of((step - 2) * top, top), top)],
                coarse_send_sem.at[layer],
                coarse_recv_sem.at[layer],
                lax.rem(me + step, patches),
                core,
            ).start()
            return carry

        lax.fori_loop(2, patches - 1, spread, 0)

    sent_far = send_far(0, nodes.at[here])
    spread_coarse(0)
    remotes = [
        remote(b[2], b[1], w_send.at[i], w_recv.at[i], me, other) for i, b in enumerate(blocks)
    ]
    for copy in remotes:
        copy.start()

    def arrive(index):
        if index:
            locals_[index].wait()
        b = blocks[index]
        remote(b[3], b[3], w_send.at[index], w_recv.at[index], me, other).wait_recv()

    def column(index, layer):
        position = index * layers + layer
        return columns[:, position : position + 1]

    waited_out = []
    sender_columns = slice(width, 2 * width)
    wide = [(k * mine // 2, (k + 1) * mine // 2) for k in range(2)]
    for layer in range(layers):
        if layer:
            arrive(place["wi", layer])
            part = dot(wi[layer, here, sender_columns], nodes[...])
            part_send[layer] = part.astype(bf16)
            sent_far = send_far(layer, part_send.at[layer])
            coarse_send[layer] = part.T[:top].astype(bf16)
            spread_coarse(layer)
        else:
            arrive(place["nodes"])
            arrive(place["wi", layer])

        own[:, :rows] = dot(wi[layer, :, sender_columns], nodes[...]).astype(bf16)
        own[:, rows:] = dot(wi[layer, :, 2 * width :], nodes[...]).astype(bf16)
        if layer == 0:
            arrive(place["edges"])
            for k in range(8):
                arrive(place["vectors"] + k)
            flat = vectors[...].reshape(8 * layers, width)
            columns[...] = flat.T
        before[...] = (
            dot(wi[layer, :, :width], edges[...]) + dot(own[...], hot_own[...]) + column(0, layer)
        )
        arrive(place["vi", layer])
        node_first = dot(vi[layer, :, :width], nodes[...]) + column(4, layer)
        arrive(place["wo", layer])
        wo_turned[...] = wo[layer].T
        arrive(place["vo", layer])
        vo_turned[...] = vo[layer].T

        relays = []

        def passed(index, ref):
            return remote(ref, ref, relay_send.at[layer, index], relay_recv.at[layer, index], me, other)

        for side in range(2):
            sent_far[side].wait_recv()
            relays.append(passed(side, halo.at[layer, here, pl.ds(side * rows, rows)]))
            relays[-1].start()
        every = coarse.at[layer, core, pl.ds(0, far * top)]
        all_coarse = remote(every, every, coarse_send_sem.at[layer], coarse_recv_sem.at[layer], me, other)
        all_coarse.wait_recv()
        relays.append(passed(2, every))
        relays[-1].start()

        if layer == 0:
            senders_here = wi[layer, :, pl.ds(pl.multiple_of(width + core * half, half), half)]
            senders_there = wi[layer, :, pl.ds(pl.multiple_of(width + other * half, half), half)]
            table[:, : 2 * rows] = dot(senders_here, halo[layer, here, :])
            table[:, 2 * rows :] = dot(senders_here, coarse[layer, core], ((1,), (1,)))
        else:
            before[here, :] = (
                before[here, :]
                + dot(halo[layer, here, :], hot_far[: 2 * rows])
                + dot(coarse[layer, core], hot_far[2 * rows :], ((0,), (0,)))
            )
        for side in range(2):
            passed(side, halo.at[layer, there, pl.ds(side * rows, rows)]).wait_recv()
        passed(2, coarse.at[layer, other, pl.ds(0, far * top)]).wait_recv()
        if layer == 0:
            near = (table[:, : 2 * rows] + dot(senders_there, halo[layer, there, :])).astype(bf16)
            away = (
                table[:, 2 * rows :] + dot(senders_there, coarse[layer, other], ((1,), (1,)))
            ).astype(bf16)
        else:
            before[there, :] = (
                before[there, :]
                + dot(halo[layer, there, :], hot_far[: 2 * rows])
                + dot(coarse[layer, other], hot_far[2 * rows :], ((0,), (0,)))
            )

        partial = None
        for low, high in wide:
            value = before[:, low:high]
            if layer == 0:
                value = (
                    value
                    + dot(near, hot_far[: 2 * rows, low:high])
                    + dot(away, hot_far[2 * rows :, low:high])
                )
            hidden = silu(value).astype(bf16)
            mlp = dot(wo_turned[...], hidden) + column(1, layer)
            updated = edges[:, low:high].astype(f32) + layer_norm(mlp, column(2, layer), column(3, layer))
            fresh = jnp.where(live[:, low:high], updated, 0.0).astype(bf16)
            edges[:, low:high] = fresh
            term = dot(fresh, incidence[:, low:high], ((1,), (1,)))
            partial = term if partial is None else partial + term
        agg_send[layer] = partial.astype(bf16)
        swap = remote(
            agg_send.at[layer], agg_recv.at[layer], agg_sems.at[layer, 0], agg_sems.at[layer, 1], me, other
        )
        swap.start()
        if layer == layers - 1:
            keep = pltpu.make_async_copy(edges.at[here], edges_out.at[:, my_slots], out_sems.at[0])
            keep.start()
            give = remote(
                edges.at[there], edges_out.at[:, my_slots], out_sems.at[1], out_sems.at[2], me, other
            )
            give.start()
        swap.wait_recv()
        aggregate = (partial + agg_recv[layer].astype(f32)).astype(bf16)
        node_hidden = silu(node_first + dot(vi[layer, :, width:], aggregate)).astype(bf16)
        node_mlp = dot(vo_turned[...], node_hidden) + column(5, layer)
        for copy in sent_far:
            copy.wait_send()
        nodes[...] = (
            nodes[...].astype(f32) + layer_norm(node_mlp, column(6, layer), column(7, layer))
        ).astype(bf16)
        waited_out += [all_coarse] + relays + [swap]

    store = pltpu.make_async_copy(nodes.at[here], nodes_out, out_sems.at[3])
    store.start()
    for copy in remotes + waited_out:
        copy.wait_send()
    keep.wait()
    give.wait_send()
    got = edges_out.at[:, other_slots]
    remote(got, got, out_sems.at[1], out_sems.at[2], me, other).wait_recv()
    store.wait()


def put(nodes, edges, nodes_out, edges_out, sems):
    copies = [
        pltpu.make_async_copy(edges, edges_out, sems.at[0]),
        pltpu.make_async_copy(nodes, nodes_out, sems.at[1]),
    ]
    for copy in copies:
        copy.start()
    for copy in copies:
        copy.wait()


def on_device(
    patches,
    node_latents,
    edge_latents,
    senders,
    receivers,
    edge_count,
    edge_in_weight,
    edge_in_bias,
    edge_out_weight,
    edge_out_bias,
    edge_gain,
    edge_shift,
    node_in_weight,
    node_in_bias,
    node_out_weight,
    node_out_bias,
    node_gain,
    node_shift,
):
    half, rows = node_latents.shape
    slots = edge_latents.shape[1]
    layers = edge_in_weight.shape[0]
    width = 2 * half
    mine = slots // 2
    top = rows // 8
    far_rows = -(-(patches - 3) * top // 128) * 128
    vmem = pltpu.VMEM
    dma = pltpu.SemaphoreType.DMA
    copies = 2 + 4 * layers + 8
    anywhere = pl.BlockSpec(memory_space=pl.ANY)
    results = pl.pallas_call(
        functools.partial(kernel, patches),
        out_shape=(
            vmem((half, rows), bf16),
            vmem((half, slots), bf16),
        ),
        in_specs=[anywhere] * 17,
        out_specs=(pl.BlockSpec(memory_space=vmem),) * 2,
        scratch_shapes=[
            vmem((width, rows), bf16),
            vmem((width, mine), bf16),
            vmem((layers, width, 3 * width), bf16),
            vmem((layers, width, width), bf16),
            vmem((layers, width, 2 * width), bf16),
            vmem((layers, width, width), bf16),
            vmem((8, layers, width), f32),
            vmem((width, 8 * layers), f32),
            vmem((layers, width, 2 * rows), bf16),
            vmem((layers, 2, far_rows, half), bf16),
            vmem((layers, half, rows), bf16),
            vmem((layers, top, half), bf16),
            vmem((layers, width, rows), bf16),
            vmem((layers, width, rows), bf16),
            vmem((width, 2 * rows), bf16),
            vmem((width, 2 * rows + far_rows), f32),
            vmem((2 * rows, mine), bf16),
            vmem((2 * rows + far_rows, mine), bf16),
            vmem((rows, mine), bf16),
            vmem((width, mine), f32),
            vmem((1, slots), jnp.int32),
            vmem((1, slots), jnp.int32),
            pltpu.SMEM((1,), jnp.int32),
            vmem((width, width), bf16),
            vmem((width, width), bf16),
            dma((3,)),
            dma((copies,)),
            dma((copies,)),
            dma((copies,)),
            dma((layers, 2)),
            dma((layers, 2)),
            dma((layers,)),
            dma((layers,)),
            dma((layers, 3)),
            dma((layers, 3)),
            dma((layers, 2)),
            dma((4,)),
        ],
        compiler_params=pltpu.CompilerParams(collective_id=0, has_side_effects=True, vmem_limit_bytes=56 * 2**20),
    )(
        node_latents,
        edge_latents,
        senders.reshape(1, slots),
        receivers.reshape(1, slots),
        edge_count,
        edge_in_weight,
        edge_out_weight,
        node_in_weight,
        node_out_weight,
        edge_in_bias,
        edge_out_bias,
        edge_gain,
        edge_shift,
        node_in_bias,
        node_out_bias,
        node_gain,
        node_shift,
    )
    return pl.pallas_call(
        put,
        out_shape=(
            jax.ShapeDtypeStruct((half, rows), bf16),
            jax.ShapeDtypeStruct((half, slots), bf16),
        ),
        in_specs=[pl.BlockSpec(memory_space=vmem)] * 2,
        out_specs=(anywhere, anywhere),
        scratch_shapes=[dma((2,))],
        compiler_params=pltpu.CompilerParams(vmem_limit_bytes=4 * 2**20),
    )(*results)


def solution(mesh):
    by_width = P(None, "width")
    return jax.shard_map(
        functools.partial(on_device, mesh.shape["patch"]),
        mesh=mesh,
        in_specs=(
            P("width", "patch"),
            P("width", "patch"),
            P("patch"),
            P("patch"),
            P("patch"),
            P(None, "width", None),
            by_width,
            P(None, "width", None),
            by_width,
            by_width,
            by_width,
            P(None, "width", None),
            by_width,
            P(None, "width", None),
            by_width,
            by_width,
            by_width,
        ),
        out_specs=(P("width", "patch"), P("width", "patch")),
        check_vma=False,
    )
```

```python
import functools

import jax
import jax.numpy as jnp
from jax import lax
from jax.experimental import pallas as pl
from jax.experimental.pallas import tpu as pltpu
from jax.sharding import PartitionSpec as P

MESH = pl.DeviceIdType.MESH
epsilon = 1e-05
bf16 = jnp.bfloat16
f32 = jnp.float32


def dot(left, right, dims=((1,), (0,))):
    return lax.dot_general(left, right, (dims, ((), ())), preferred_element_type=f32)


def silu(v):
    h = 0.5 * v
    return h + h * jnp.tanh(h)


def layer_norm(values, gain, shift):
    width = values.shape[0]
    mean = jnp.sum(values, axis=0, keepdims=True) / width
    square = jnp.sum(values * values, axis=0, keepdims=True) / width
    return (values - mean) * lax.rsqrt(square - mean * mean + epsilon) * gain + shift


def kernel(
    patches,
    nodes_in,
    edges_in,
    senders_in,
    receivers_in,
    count_in,
    wi_in,
    wo_in,
    vi_in,
    vo_in,
    *rest,
):
    vector_in = rest[:8]
    nodes_out, edges_out = rest[8:10]
    (
        nodes,
        edges,
        wi,
        wo,
        vi,
        vo,
        vectors,
        columns,
        halo,
        coarse,
        part_send,
        coarse_send,
        agg_send,
        agg_recv,
        own,
        table,
        hot_own,
        hot_far,
        incidence,
        before,
        senders_ref,
        receivers_ref,
        count_ref,
        wo_turned,
        vo_turned,
        graph_sem,
        local_sem,
        w_send,
        w_recv,
        halo_send,
        halo_recv,
        coarse_send_sem,
        coarse_recv_sem,
        relay_send,
        relay_recv,
        agg_sems,
        out_sems,
    ) = rest[10:]
    layers = wi.shape[0]
    half = nodes_in.shape[0]
    width = 2 * half
    rows = nodes_in.shape[1]
    slots = edges_in.shape[1]
    mine = slots // 2
    top = coarse_send.shape[1]
    far = patches - 3

    me = lax.axis_index("patch")
    core = lax.axis_index("width")
    other = 1 - core
    here = pl.ds(pl.multiple_of(core * half, half), half)
    there = pl.ds(pl.multiple_of(other * half, half), half)
    my_slots = pl.ds(pl.multiple_of(core * mine, mine), mine)
    other_slots = pl.ds(pl.multiple_of(other * mine, mine), mine)

    def local(src, dst, index):
        return pltpu.make_async_copy(src, dst, local_sem.at[index])

    def remote(src, dst, send, recv, patch, width_index):
        return pltpu.make_async_remote_copy(
            src_ref=src,
            dst_ref=dst,
            send_sem=send,
            recv_sem=recv,
            device_id={"patch": patch, "width": width_index},
            device_id_type=MESH,
        )

    blocks = [
        (nodes_in, nodes.at[here], nodes_in, nodes.at[there]),
        (edges_in.at[:, my_slots], edges.at[here], edges_in.at[:, other_slots], edges.at[there]),
    ]
    place = {"nodes": 0, "edges": 1}
    for layer in range(layers):
        for name, source, target in (("wi", wi_in, wi), ("wo", wo_in, wo), ("vi", vi_in, vi), ("vo", vo_in, vo)):
            place[name, layer] = len(blocks)
            blocks.append(
                (source.at[layer], target.at[layer, here], source.at[layer], target.at[layer, there])
            )
        if layer == 0:
            place["vectors"] = len(blocks)
            for index, source in enumerate(vector_in):
                blocks.append(
                    (source, vectors.at[index, :, here], source, vectors.at[index, :, there])
                )

    def greet(step, carry):
        target = lax.rem(me + step, patches)
        pl.semaphore_signal(
            pltpu.get_barrier_semaphore(), inc=1, device_id={"patch": target, "width": core}, device_id_type=MESH
        )
        return carry

    barrier = pltpu.get_barrier_semaphore()
    pl.semaphore_signal(barrier, inc=1, device_id={"patch": me, "width": other}, device_id_type=MESH)
    lax.fori_loop(1, patches, greet, 0)

    graph = [
        pltpu.make_async_copy(source, target, graph_sem.at[i])
        for i, (source, target) in enumerate(
            ((senders_in, senders_ref), (receivers_in, receivers_ref), (count_in, count_ref))
        )
    ]
    locals_ = [local(b[0], b[1], i) for i, b in enumerate(blocks)]
    locals_[0].start()
    for copy in graph + locals_[1:]:
        copy.start()
    locals_[0].wait()
    coarse_send[0] = nodes[here, :].astype(f32).T[:top].astype(bf16)
    for copy in graph:
        copy.wait()

    sender = senders_ref[:, my_slots]
    receiver = receivers_ref[:, my_slots] - me * rows
    slot = lax.broadcasted_iota(jnp.int32, (1, mine), 1) + core * mine
    live = slot < count_ref[0]
    owner = sender // rows
    within = sender - owner * rows
    distance = lax.rem(me - owner + patches, patches)
    node_iota = lax.broadcasted_iota(jnp.int32, (rows, mine), 0)

    def hot(index, iota):
        return jnp.where(iota == index, 1.0, 0.0).astype(bf16)

    hot_own[:rows] = hot(jnp.where(distance == 0, within, -1), node_iota)
    hot_own[rows:] = hot(receiver, node_iota)
    hot_far[:rows] = hot(jnp.where(distance == 1, within, -1), node_iota)
    hot_far[rows : 2 * rows] = hot(jnp.where(distance == patches - 1, within, -1), node_iota)
    far_index = jnp.where((distance >= 2) & (distance <= patches - 2), (distance - 2) * top + within, -1)
    hot_far[2 * rows :] = hot(far_index, lax.broadcasted_iota(jnp.int32, (coarse.shape[2], mine), 0))
    incidence[...] = hot(jnp.where(live, receiver, -1), node_iota)
    pad = coarse.shape[2] - far * top
    if pad:
        for layer in range(layers):
            for part in range(2):
                coarse[layer, part, far * top :, :] = jnp.zeros((pad, half), bf16)

    pl.semaphore_wait(barrier, patches)

    def send_far(layer, source):
        copies = [
            remote(
                source,
                halo.at[layer, here, pl.ds(side * rows, rows)],
                halo_send.at[layer, side],
                halo_recv.at[layer, side],
                lax.rem(me + step, patches),
                core,
            )
            for side, step in enumerate((1, patches - 1))
        ]
        for copy in copies:
            copy.start()
        return copies

    def spread_coarse(layer):
        def spread(step, carry):
            remote(
                coarse_send.at[layer],
                coarse.at[layer, core, pl.ds(pl.multiple_of((step - 2) * top, top), top)],
                coarse_send_sem.at[layer],
                coarse_recv_sem.at[layer],
                lax.rem(me + step, patches),
                core,
            ).start()
            return carry

        lax.fori_loop(2, patches - 1, spread, 0)

    sent_far = send_far(0, nodes.at[here])
    spread_coarse(0)
    remotes = [
        remote(b[2], b[1], w_send.at[i], w_recv.at[i], me, other) for i, b in enumerate(blocks)
    ]
    for copy in remotes:
        copy.start()

    def arrive(index):
        if index:
            locals_[index].wait()
        b = blocks[index]
        remote(b[3], b[3], w_send.at[index], w_recv.at[index], me, other).wait_recv()

    def column(index, layer):
        position = index * layers + layer
        return columns[:, position : position + 1]

    waited_out = []
    sender_columns = slice(width, 2 * width)
    wide = [(k * mine // 2, (k + 1) * mine // 2) for k in range(2)]
    for layer in range(layers):
        if layer:
            arrive(place["wi", layer])
            part = dot(wi[layer, here, sender_columns], nodes[...])
            part_send[layer] = part.astype(bf16)
            sent_far = send_far(layer, part_send.at[layer])
            coarse_send[layer] = part.T[:top].astype(bf16)
            spread_coarse(layer)
        else:
            arrive(place["nodes"])
            arrive(place["wi", layer])

        own[:, :rows] = dot(wi[layer, :, sender_columns], nodes[...]).astype(bf16)
        own[:, rows:] = dot(wi[layer, :, 2 * width :], nodes[...]).astype(bf16)
        if layer == 0:
            arrive(place["edges"])
            for k in range(8):
                arrive(place["vectors"] + k)
            flat = vectors[...].reshape(8 * layers, width)
            columns[...] = flat.T
        before[...] = (
            dot(wi[layer, :, :width], edges[...]) + dot(own[...], hot_own[...]) + column(0, layer)
        )
        arrive(place["vi", layer])
        node_first = dot(vi[layer, :, :width], nodes[...]) + column(4, layer)
        arrive(place["wo", layer])
        wo_turned[...] = wo[layer].T
        arrive(place["vo", layer])
        vo_turned[...] = vo[layer].T

        relays = []

        def passed(index, ref):
            return remote(ref, ref, relay_send.at[layer, index], relay_recv.at[layer, index], me, other)

        for side in range(2):
            sent_far[side].wait_recv()
            relays.append(passed(side, halo.at[layer, here, pl.ds(side * rows, rows)]))
            relays[-1].start()
        every = coarse.at[layer, core, pl.ds(0, far * top)]
        all_coarse = remote(every, every, coarse_send_sem.at[layer], coarse_recv_sem.at[layer], me, other)
        all_coarse.wait_recv()
        relays.append(passed(2, every))
        relays[-1].start()

        if layer == 0:
            senders_here = wi[layer, :, pl.ds(pl.multiple_of(width + core * half, half), half)]
            senders_there = wi[layer, :, pl.ds(pl.multiple_of(width + other * half, half), half)]
            table[:, : 2 * rows] = dot(senders_here, halo[layer, here, :])
            table[:, 2 * rows :] = dot(senders_here, coarse[layer, core], ((1,), (1,)))
        else:
            before[here, :] = (
                before[here, :]
                + dot(halo[layer, here, :], hot_far[: 2 * rows])
                + dot(coarse[layer, core], hot_far[2 * rows :], ((0,), (0,)))
            )
        for side in range(2):
            passed(side, halo.at[layer, there, pl.ds(side * rows, rows)]).wait_recv()
        passed(2, coarse.at[layer, other, pl.ds(0, far * top)]).wait_recv()
        if layer == 0:
            near = (table[:, : 2 * rows] + dot(senders_there, halo[layer, there, :])).astype(bf16)
            away = (
                table[:, 2 * rows :] + dot(senders_there, coarse[layer, other], ((1,), (1,)))
            ).astype(bf16)
        else:
            before[there, :] = (
                before[there, :]
                + dot(halo[layer, there, :], hot_far[: 2 * rows])
                + dot(coarse[layer, other], hot_far[2 * rows :], ((0,), (0,)))
            )

        partial = None
        for low, high in wide:
            value = before[:, low:high]
            if layer == 0:
                value = (
                    value
                    + dot(near, hot_far[: 2 * rows, low:high])
                    + dot(away, hot_far[2 * rows :, low:high])
                )
            hidden = silu(value).astype(bf16)
            mlp = dot(wo_turned[...], hidden) + column(1, layer)
            updated = edges[:, low:high].astype(f32) + layer_norm(mlp, column(2, layer), column(3, layer))
            fresh = jnp.where(live[:, low:high], updated, 0.0).astype(bf16)
            edges[:, low:high] = fresh
            term = dot(fresh, incidence[:, low:high], ((1,), (1,)))
            partial = term if partial is None else partial + term
        agg_send[layer] = partial.astype(bf16)
        swap = remote(
            agg_send.at[layer], agg_recv.at[layer], agg_sems.at[layer, 0], agg_sems.at[layer, 1], me, other
        )
        swap.start()
        if layer == layers - 1:
            keep = pltpu.make_async_copy(edges.at[here], edges_out.at[:, my_slots], out_sems.at[0])
            keep.start()
            give = remote(
                edges.at[there], edges_out.at[:, my_slots], out_sems.at[1], out_sems.at[2], me, other
            )
            give.start()
        swap.wait_recv()
        aggregate = (partial + agg_recv[layer].astype(f32)).astype(bf16)
        node_hidden = silu(node_first + dot(vi[layer, :, width:], aggregate)).astype(bf16)
        node_mlp = dot(vo_turned[...], node_hidden) + column(5, layer)
        for copy in sent_far:
            copy.wait_send()
        nodes[...] = (
            nodes[...].astype(f32) + layer_norm(node_mlp, column(6, layer), column(7, layer))
        ).astype(bf16)
        waited_out += [all_coarse] + relays + [swap]

    nodes_out[...] = nodes[here, :]
    for copy in remotes + waited_out:
        copy.wait_send()
    keep.wait()
    give.wait_send()
    got = edges_out.at[:, other_slots]
    remote(got, got, out_sems.at[1], out_sems.at[2], me, other).wait_recv()


def put(nodes, edges, nodes_out, edges_out, sems):
    copies = [
        pltpu.make_async_copy(edges, edges_out, sems.at[0]),
        pltpu.make_async_copy(nodes, nodes_out, sems.at[1]),
    ]
    for copy in copies:
        copy.start()
    for copy in copies:
        copy.wait()


def on_device(
    patches,
    node_latents,
    edge_latents,
    senders,
    receivers,
    edge_count,
    edge_in_weight,
    edge_in_bias,
    edge_out_weight,
    edge_out_bias,
    edge_gain,
    edge_shift,
    node_in_weight,
    node_in_bias,
    node_out_weight,
    node_out_bias,
    node_gain,
    node_shift,
):
    half, rows = node_latents.shape
    slots = edge_latents.shape[1]
    layers = edge_in_weight.shape[0]
    width = 2 * half
    mine = slots // 2
    top = rows // 8
    far_rows = -(-(patches - 3) * top // 128) * 128
    vmem = pltpu.VMEM
    dma = pltpu.SemaphoreType.DMA
    copies = 2 + 4 * layers + 8
    anywhere = pl.BlockSpec(memory_space=pl.ANY)
    results = pl.pallas_call(
        functools.partial(kernel, patches),
        out_shape=(
            vmem((half, rows), bf16),
            vmem((half, slots), bf16),
        ),
        in_specs=[anywhere] * 17,
        out_specs=(pl.BlockSpec(memory_space=vmem),) * 2,
        scratch_shapes=[
            vmem((width, rows), bf16),
            vmem((width, mine), bf16),
            vmem((layers, width, 3 * width), bf16),
            vmem((layers, width, width), bf16),
            vmem((layers, width, 2 * width), bf16),
            vmem((layers, width, width), bf16),
            vmem((8, layers, width), f32),
            vmem((width, 8 * layers), f32),
            vmem((layers, width, 2 * rows), bf16),
            vmem((layers, 2, far_rows, half), bf16),
            vmem((layers, half, rows), bf16),
            vmem((layers, top, half), bf16),
            vmem((layers, width, rows), bf16),
            vmem((layers, width, rows), bf16),
            vmem((width, 2 * rows), bf16),
            vmem((width, 2 * rows + far_rows), f32),
            vmem((2 * rows, mine), bf16),
            vmem((2 * rows + far_rows, mine), bf16),
            vmem((rows, mine), bf16),
            vmem((width, mine), f32),
            vmem((1, slots), jnp.int32),
            vmem((1, slots), jnp.int32),
            pltpu.SMEM((1,), jnp.int32),
            vmem((width, width), bf16),
            vmem((width, width), bf16),
            dma((3,)),
            dma((copies,)),
            dma((copies,)),
            dma((copies,)),
            dma((layers, 2)),
            dma((layers, 2)),
            dma((layers,)),
            dma((layers,)),
            dma((layers, 3)),
            dma((layers, 3)),
            dma((layers, 2)),
            dma((3,)),
        ],
        compiler_params=pltpu.CompilerParams(collective_id=0, has_side_effects=True, vmem_limit_bytes=56 * 2**20),
    )(
        node_latents,
        edge_latents,
        senders.reshape(1, slots),
        receivers.reshape(1, slots),
        edge_count,
        edge_in_weight,
        edge_out_weight,
        node_in_weight,
        node_out_weight,
        edge_in_bias,
        edge_out_bias,
        edge_gain,
        edge_shift,
        node_in_bias,
        node_out_bias,
        node_gain,
        node_shift,
    )
    return pl.pallas_call(
        put,
        out_shape=(
            jax.ShapeDtypeStruct((half, rows), bf16),
            jax.ShapeDtypeStruct((half, slots), bf16),
        ),
        in_specs=[pl.BlockSpec(memory_space=vmem)] * 2,
        out_specs=(anywhere, anywhere),
        scratch_shapes=[dma((2,))],
        compiler_params=pltpu.CompilerParams(vmem_limit_bytes=4 * 2**20),
    )(*results)


def solution(mesh):
    by_width = P(None, "width")
    return jax.shard_map(
        functools.partial(on_device, mesh.shape["patch"]),
        mesh=mesh,
        in_specs=(
            P("width", "patch"),
            P("width", "patch"),
            P("patch"),
            P("patch"),
            P("patch"),
            P(None, "width", None),
            by_width,
            P(None, "width", None),
            by_width,
            by_width,
            by_width,
            P(None, "width", None),
            by_width,
            P(None, "width", None),
            by_width,
            by_width,
            by_width,
        ),
        out_specs=(P("width", "patch"), P("width", "patch")),
        check_vma=False,
    )
```
